32 devices in a mesh: dp: 4 (over z), tp: 8 (over y, x, core).
Axes of the slice: x: 2, y: 2, z: 4, core: 2. Of those that a mesh axis runs over, the one named last changes fastest.
Arguments:
- x_resid: bfloat16 [24, 1024, 5120], P('dp', 'tp'), parts along dimension 0
- positions: int32 [24, 1024], P('dp', 'tp'), parts along dimension 0
- norm_gain: bfloat16 [5120], replicated
- w_q: bfloat16 [5120, 5120], P(None, 'tp')
- w_k: bfloat16 [5120, 1024], P(None, 'tp')
- w_v: bfloat16 [5120, 1024], P(None, 'tp')
- q_gain: bfloat16 [128], replicated
- k_gain: bfloat16 [128], replicated
- w_o: bfloat16 [5120, 5120], P('tp')
Outputs:
- output: bfloat16 [24, 1024, 5120], P('dp', 'tp'), parts along dimension 0
There are 4 independent parts. The reference program is written for one: setup_inputs(seed, part) draws one part's arguments, and reference() takes and returns one part's arrays. A program takes and returns all parts, laid end to end along the dimension named above; an argument that names none is the same for every part.
All inputs are finite; a program needn't handle non-finite values.
Results may differ from the reference program's by a relative error of at most 0.0113421.
Values are sent between devices in bfloat16 or wider.
A program may use at most 1 GiB of HBM per device.

```python
import jax
import jax.numpy as jnp
from jax import lax

BATCH = 6
SEQ_LEN = 1024
D_MODEL = 5120
HEADS = 40
KV_HEADS = 8
HEAD_DIM = 128
Q_BLOCK = 128

GROUP_SIZE = HEADS // KV_HEADS
EPS = 1e-6
THETA = 1000000.0


def setup_inputs(seed: int = 0, part: int = 0) -> dict:
    base_key = jax.random.key(seed)
    shared_keys = jax.random.split(base_key, 8)
    part_keys = jax.random.split(jax.random.fold_in(base_key, part), 3)
    x_in = jax.random.normal(part_keys[0], (BATCH, SEQ_LEN, D_MODEL), jnp.float32)
    start_pos = jax.random.randint(part_keys[1], (BATCH, 1), 0, 1024)
    pos_steps = jax.random.randint(part_keys[2], (BATCH, SEQ_LEN), 1, 4)
    pos_vals = (start_pos + jnp.cumsum(pos_steps, axis=1)).astype(jnp.int32)
    proj_scale = D_MODEL ** -0.5
    out_scale = (HEADS * HEAD_DIM) ** -0.5
    return {
        'x_resid': x_in.astype(jnp.bfloat16),
        'positions': pos_vals,
        'norm_gain': jax.random.uniform(shared_keys[0], (D_MODEL,), jnp.float32, 0.5, 1.5).astype(jnp.bfloat16),
        'w_q': (jax.random.normal(shared_keys[1], (D_MODEL, HEADS * HEAD_DIM), jnp.float32) * proj_scale).astype(jnp.bfloat16),
        'w_k': (jax.random.normal(shared_keys[2], (D_MODEL, KV_HEADS * HEAD_DIM), jnp.float32) * proj_scale).astype(jnp.bfloat16),
        'w_v': (jax.random.normal(shared_keys[3], (D_MODEL, KV_HEADS * HEAD_DIM), jnp.float32) * proj_scale).astype(jnp.bfloat16),
        'q_gain': jax.random.uniform(shared_keys[4], (HEAD_DIM,), jnp.float32, 1.2, 2.0).astype(jnp.bfloat16),
        'k_gain': jax.random.uniform(shared_keys[5], (HEAD_DIM,), jnp.float32, 1.2, 2.0).astype(jnp.bfloat16),
        'w_o': (jax.random.normal(shared_keys[6], (HEADS * HEAD_DIM, D_MODEL), jnp.float32) * out_scale).astype(jnp.bfloat16),
    }


def rms_scale(vals, gain):
    mean_sq = jnp.mean(vals * vals, axis=-1, keepdims=True)
    return vals * lax.rsqrt(mean_sq + EPS) * gain.astype(jnp.float32)


def rotate_half(vals, cos_t, sin_t):
    half_dim = HEAD_DIM // 2
    lower_half = vals[..., :half_dim]
    upper_half = vals[..., half_dim:]
    return jnp.concatenate([lower_half * cos_t - upper_half * sin_t, upper_half * cos_t + lower_half * sin_t], axis=-1)


def reference(x_resid, positions, norm_gain, w_q, w_k, w_v, q_gain, k_gain, w_o):
    inv_freq = THETA ** (-(jnp.arange(HEAD_DIM // 2, dtype=jnp.float32) * (2.0 / HEAD_DIM)))
    key_index = jnp.arange(SEQ_LEN)
    block_starts = jnp.arange(SEQ_LEN // Q_BLOCK) * Q_BLOCK

    def one_sequence(seq_args):
        x_seq, pos_seq = seq_args
        x_f32 = x_seq.astype(jnp.float32)
        normed = rms_scale(x_f32, norm_gain).astype(jnp.bfloat16)
        q_proj = jnp.dot(normed, w_q, preferred_element_type=jnp.float32).astype(jnp.bfloat16)
        k_proj = jnp.dot(normed, w_k, preferred_element_type=jnp.float32).astype(jnp.bfloat16)
        v_proj = jnp.dot(normed, w_v, preferred_element_type=jnp.float32).astype(jnp.bfloat16)
        angles = pos_seq.astype(jnp.float32)[:, None] * inv_freq
        cos_t = jnp.cos(angles)
        sin_t = jnp.sin(angles)
        q_heads = q_proj.reshape(SEQ_LEN, KV_HEADS, GROUP_SIZE, HEAD_DIM).astype(jnp.float32)
        k_heads = k_proj.reshape(SEQ_LEN, KV_HEADS, HEAD_DIM).astype(jnp.float32)
        q_rot = rotate_half(rms_scale(q_heads, q_gain), cos_t[:, None, None, :], sin_t[:, None, None, :]).astype(jnp.bfloat16)
        k_rot = rotate_half(rms_scale(k_heads, k_gain), cos_t[:, None, :], sin_t[:, None, :]).astype(jnp.bfloat16)
        k_wide = k_rot.astype(jnp.float32)
        v_wide = v_proj.reshape(SEQ_LEN, KV_HEADS, HEAD_DIM).astype(jnp.float32)
        q_blocks = q_rot.reshape(SEQ_LEN // Q_BLOCK, Q_BLOCK, KV_HEADS, GROUP_SIZE, HEAD_DIM)

        def one_block(block_args):
            q_block, block_start = block_args
            scores = jnp.einsum('qkgh,tkh->kgqt', q_block.astype(jnp.float32), k_wide) * (HEAD_DIM ** -0.5)
            query_index = block_start + jnp.arange(Q_BLOCK)
            allowed = query_index[:, None] >= key_index[None, :]
            scores = jnp.where(allowed, scores, -jnp.inf)
            attn_probs = jax.nn.softmax(scores, axis=-1).astype(jnp.bfloat16)
            mixed = jnp.einsum('kgqt,tkh->qkgh', attn_probs.astype(jnp.float32), v_wide)
            return mixed.astype(jnp.bfloat16)

        attn_out = lax.map(one_block, (q_blocks, block_starts)).reshape(SEQ_LEN, HEADS * HEAD_DIM)
        attn_sum = jnp.dot(attn_out, w_o, preferred_element_type=jnp.float32)
        return (x_f32 + attn_sum).astype(jnp.bfloat16)

    return lax.map(one_sequence, (x_resid, positions))
```

```python
import functools

import jax
import jax.numpy as jnp
from jax import lax
from jax.experimental import pallas as pl
from jax.experimental.pallas import tpu as pltpu
from jax.sharding import PartitionSpec as P

EPS = 1e-6
THETA = 1000000.0
LOG2E = 1.4426950408889634
NUM_GROUPS = 3


def rms_scale(vals, gain):
    mean_sq = jnp.mean(vals * vals, axis=-1, keepdims=True)
    return vals * lax.rsqrt(mean_sq + EPS) * gain.astype(jnp.float32)


def rope_tables(pos_vals, head_dim):
    inv_freq = THETA ** (-(jnp.arange(head_dim // 2, dtype=jnp.float32) * (2.0 / head_dim)))
    angles = pos_vals.astype(jnp.float32)[..., None] * inv_freq
    cos_t, sin_t = jnp.cos(angles), jnp.sin(angles)
    return jnp.concatenate([cos_t, cos_t], axis=-1), jnp.concatenate([-sin_t, sin_t], axis=-1)


def norm_rope(proj, gain, cos_t, sin_t):
    vals = rms_scale(proj.astype(jnp.float32), gain)
    half_dim = vals.shape[-1] // 2
    swapped = jnp.concatenate([vals[..., half_dim:], vals[..., :half_dim]], axis=-1)
    return (vals * cos_t + swapped * sin_t).astype(jnp.bfloat16)


def attention_kernel(group_size, offs_ref, q_ref, cos_ref, sin_ref, gain_ref, own_ref, far_ref, out_ref, k_all, v_all):
    rows, head_dim = cos_ref.shape[1], cos_ref.shape[2]
    half_blocks = own_ref.shape[2] // rows
    seq_len = 2 * half_blocks * rows
    step = seq_len // 4
    piece = pl.program_id(1)

    @pl.when(piece == 0)
    def _():
        for blk in range(half_blocks):
            for src, first in ((own_ref, 0), (far_ref, half_blocks)):
                at = pl.ds(pl.multiple_of(offs_ref[first + blk], rows), rows)
                k_all[at, :] = src[0, 0, blk * rows:(blk + 1) * rows, :]
                v_all[at, :] = src[1, 0, blk * rows:(blk + 1) * rows, :]

    cos_t, sin_t = cos_ref[0], sin_ref[0]
    gain = gain_ref[...].astype(jnp.float32)
    heads = []
    for head in range(group_size):
        u = q_ref[0, :, head * head_dim:(head + 1) * head_dim].astype(jnp.float32)
        w = u * lax.rsqrt(jnp.mean(u * u, axis=-1, keepdims=True) + EPS) * gain
        heads.append((w * cos_t + pltpu.roll(w, head_dim // 2, 1) * sin_t).astype(jnp.bfloat16))
    q_all = jnp.concatenate(heads, axis=0)
    scale = head_dim ** -0.5 * LOG2E
    start = offs_ref[piece]
    mask_one = (start % step) + lax.broadcasted_iota(jnp.int32, (rows, step), 0) >= lax.broadcasted_iota(jnp.int32, (rows, step), 1)
    mask = jnp.concatenate([mask_one] * group_size, axis=0)

    for part in range(4):
        keys = (part + 1) * step

        @pl.when(start // step == part)
        def _(keys=keys):
            scores = lax.dot_general(q_all, k_all[:keys, :], (((1,), (1,)), ((), ())), preferred_element_type=jnp.float32)
            last = jnp.where(mask, scores[:, keys - step:], -jnp.inf)
            scores = last if keys == step else jnp.concatenate([scores[:, :keys - step], last], axis=1)
            peak = jnp.max(scores, axis=-1, keepdims=True)
            exps = jnp.exp2((scores - peak) * scale)
            inv = 1.0 / jnp.sum(exps, axis=-1, keepdims=True)
            probs = (exps * inv).astype(jnp.bfloat16)
            mixed = jnp.dot(probs, v_all[:keys, :], preferred_element_type=jnp.float32).astype(jnp.bfloat16)
            for head in range(group_size):
                out_ref[0, :, head * head_dim:(head + 1) * head_dim] = mixed[head * rows:(head + 1) * rows]


def attention(offs, q, cos_t, sin_t, gain, own, far, rows):
    batch, tokens, width = q.shape
    head_dim = gain.shape[-1]
    per_row = lambda last: pl.BlockSpec((1, rows, last), lambda b, i, offs_ref: (b, i, 0))
    keys = pl.BlockSpec((2, 1, tokens, head_dim), lambda b, i, offs_ref: (0, b, 0, 0))
    flops = batch * tokens * 2 * tokens * width * 4
    return pl.pallas_call(
        functools.partial(attention_kernel, width // head_dim),
        grid_spec=pltpu.PrefetchScalarGridSpec(
            num_scalar_prefetch=1,
            grid=(batch, tokens // rows),
            in_specs=[per_row(width), per_row(head_dim), per_row(head_dim),
                      pl.BlockSpec((1, head_dim), lambda b, i, offs_ref: (0, 0)), keys, keys],
            out_specs=per_row(width),
            scratch_shapes=[pltpu.VMEM((2 * tokens, head_dim), jnp.bfloat16)] * 2,
        ),
        out_shape=jax.ShapeDtypeStruct(q.shape, jnp.bfloat16),
        cost_estimate=pl.CostEstimate(flops=3 * flops, bytes_accessed=q.size * 4, transcendentals=0),
        compiler_params=pltpu.CompilerParams(dimension_semantics=("arbitrary", "arbitrary")),
        name="attention",
    )(offs, q, cos_t, sin_t, gain.reshape(1, head_dim), own, far)


def tie(value, *deps):
    return lax.optimization_barrier((value, *deps))[0]


def dot32(a, b):
    return lax.dot_general(a, b, (((a.ndim - 1,), (0,)), ((), ())), preferred_element_type=jnp.float32)


def solution(mesh):
    dp, tp = mesh.shape['dp'], mesh.shape['tp']
    axes = ('dp', 'tp')

    def permutation(move):
        pairs = []
        for src in range(dp * tp):
            z, r = divmod(src, tp)
            z, y, x, c = move(z, r >> 2, (r >> 1) & 1, r & 1)
            pairs.append((src, z * tp + y * 4 + x * 2 + c))
        return pairs

    perm_x = permutation(lambda z, y, x, c: (z, y, 1 - x, c))
    perm_y = permutation(lambda z, y, x, c: (z, 1 - y, x, c))
    perm_z = permutation(lambda z, y, x, c: (z ^ 1, y, x, c))
    perm_c = permutation(lambda z, y, x, c: (z, y, x, 1 - c))
    send = lambda arr, perm: lax.ppermute(arr, axes, perm)

    def local_block(x_loc, pos_loc, norm_gain, w_q, w_k, w_v, q_gain, k_gain, w_o):
        batch, piece, width = x_loc.shape
        head_dim = q_gain.shape[0]
        per_group = batch // NUM_GROUPS
        q_cols = w_q.shape[1]
        rank = lax.axis_index('tp')
        y_idx, x_idx, c_idx = rank // 4, (rank // 2) % 2, rank % 2
        parity = lax.axis_index('dp') % 2

        groups = [slice(g * per_group, (g + 1) * per_group) for g in range(NUM_GROUPS)]
        half = width // 2

        def normed(g):
            return rms_scale(x_loc[groups[g]].astype(jnp.float32), norm_gain).astype(jnp.bfloat16)

        def own_half(w, row, rows, col, cols):
            return lax.dynamic_slice(w, (row + parity * (rows // 2), col), (rows // 2, cols))

        def assemble(direct, passed):
            return jnp.concatenate([jnp.where(parity == 0, direct, passed), jnp.where(parity == 0, passed, direct)], axis=0)

        pos_y = send(pos_loc, perm_y)
        n_own = [normed(0)]
        n_y = [send(tie(n_own[0], pos_y), perm_y)]
        w_kv = jnp.concatenate([w_k, w_v], axis=1)
        kv_direct = send(own_half(w_kv, 0, width, 0, 2 * head_dim), perm_x)
        q_direct = [send(own_half(w_q, 0, half, 0, q_cols), perm_x)]
        for g in range(1, NUM_GROUPS):
            n_own.append(normed(g))
            n_y.append(send(n_own[g], perm_y))
        q_direct.append(send(own_half(w_q, half, half, 0, q_cols), perm_x))
        o_direct = [send(own_half(w_o, 0, q_cols, 0, half), perm_x)]

        pos_a = jnp.concatenate([pos_loc, pos_y], axis=1)
        pos_all = jnp.concatenate([pos_a, send(pos_a, perm_c)], axis=1)
        cos_t, sin_t = rope_tables(pos_all, head_dim)

        def piece_start(y, x, c):
            return (y * 4 + x * 2 + c) * piece

        offs = jnp.stack([piece_start(yy, xx, cc) for xx in (x_idx, 1 - x_idx) for cc in (c_idx, 1 - c_idx) for yy in (y_idx, 1 - y_idx)]).astype(jnp.int32)

        kv_passed = send(kv_direct, perm_z)

        def gather(g, *deps):
            n_a = jnp.concatenate([n_own[g], n_y[g]], axis=1)
            if deps:
                n_a = tie(n_a, *deps)
            return n_a, send(n_a, perm_c)

        def project(ns, w):
            return jnp.concatenate([dot32(n, w).astype(jnp.bfloat16) for n in ns], axis=1)

        def keys_values(ns, g, w):
            kv = project(ns, w)
            pairs = []
            for s in range(2):
                k_raw = kv[..., 2 * s * head_dim:(2 * s + 1) * head_dim]
                k_rot = norm_rope(k_raw, k_gain, cos_t[groups[g]], sin_t[groups[g]])
                pairs.append(jnp.stack([k_rot, kv[..., (2 * s + 1) * head_dim:(2 * s + 2) * head_dim]]))
            own, far = pairs
            return own, far, send(far, perm_x), send(own, perm_x)

        def attend(g, s, q, kvs):
            return attention(offs, q, cos_t[groups[g]], sin_t[groups[g]], q_gain, kvs[s], kvs[2 + s], piece)

        def mix_out(o, w, *deps):
            if deps:
                o = tie(o, *deps)
            theirs = dot32(o[:, 2 * piece:], w).astype(jnp.bfloat16)
            got = send(theirs, perm_c)
            mine = dot32(tie(o[:, :2 * piece], theirs), w).astype(jnp.bfloat16)
            mine = tie(mine, got)
            both = (mine.astype(jnp.float32) + got.astype(jnp.float32)).astype(jnp.bfloat16)
            return both, send(both[:, piece:], perm_y)

        ns0 = gather(0, kv_passed)
        q1_passed = send(tie(q_direct[0], ns0[0]), perm_z)
        w_kv_all = jnp.concatenate([w_kv, assemble(kv_direct, kv_passed)], axis=1)
        kvs0 = keys_values(ns0, 0, w_kv_all)
        q_own0 = project([tie(n, kvs0[0], q1_passed) for n in ns0], w_q)
        q2_passed = send(tie(q_direct[1], q_own0), perm_z)
        ns1 = gather(1, q2_passed)
        kvs1 = keys_values(ns1, 1, w_kv_all)
        o_direct.append(send(tie(own_half(w_o, 0, q_cols, half, half), kvs1[0]), perm_x))
        o1_passed = send(tie(o_direct[0], kvs1[0]), perm_z)
        q_own1 = project([tie(n, kvs1[0]) for n in ns1], w_q)
        w_q_far = tie(jnp.concatenate([assemble(q_direct[0], q1_passed), assemble(q_direct[1], q2_passed)], axis=0), q_own1)
        q_far0 = project(ns0, w_q_far)
        o_own0 = attend(0, 0, tie(q_own0, q_far0), kvs0)
        o_far0 = attend(0, 1, tie(q_far0, o_own0), kvs0)
        o0 = jnp.concatenate([o_own0, o_far0], axis=-1)
        w_o_a = jnp.concatenate([w_o[:, :half], assemble(o_direct[0], o1_passed)], axis=0)
        r00 = mix_out(o0, w_o_a)
        ns2 = gather(2, r00[0])
        kvs2 = keys_values(ns2, 2, w_kv_all)
        q_far1 = project([tie(n, kvs2[0]) for n in ns1], w_q_far)
        o_own1 = attend(1, 0, tie(q_own1, q_far1), kvs1)
        o_far1 = attend(1, 1, tie(q_far1, o_own1), kvs1)
        o1 = jnp.concatenate([o_own1, o_far1], axis=-1)
        r10 = mix_out(o1, w_o_a)
        o2_passed = send(tie(o_direct[1], r10[0]), perm_z)
        q_own2 = project([tie(n, r10[0]) for n in ns2], w_q)
        q_far2 = project([tie(n, q_own2) for n in ns2], w_q_far)
        o_own2 = attend(2, 0, tie(q_own2, q_far2), kvs2)
        o_far2 = attend(2, 1, tie(q_far2, o_own2), kvs2)
        o2 = jnp.concatenate([o_own2, o_far2], axis=-1)
        r20 = mix_out(o2, w_o_a)
        w_o_b = tie(jnp.concatenate([w_o[:, half:], assemble(o_direct[1], o2_passed)], axis=0), r20[0])
        r01 = mix_out(o0, w_o_b)
        r11 = mix_out(o1, w_o_b, r01[0])
        r21 = mix_out(o2, w_o_b, r11[0])

        outs = []
        for g, parts in enumerate(((r00, r01), (r10, r11), (r20, r21))):
            total = jnp.concatenate([both[:, :piece].astype(jnp.float32) + final.astype(jnp.float32) for both, final in parts], axis=-1)
            outs.append((x_loc[groups[g]].astype(jnp.float32) + total).astype(jnp.bfloat16))
        return jnp.concatenate(outs, axis=0)

    return jax.shard_map(local_block, mesh=mesh, in_specs=(P('dp', 'tp', None), P('dp', 'tp'), P(None), P(None, 'tp'), P(None, 'tp'), P(None, 'tp'), P(None), P(None), P('tp', None)), out_specs=P('dp', 'tp', None), check_vma=False)
```
